32 devices in a mesh: member: 2 (over y), wave: 4 (over x, core), lev: 4 (over z).
Axes of the slice: x: 2, y: 2, z: 4, core: 2. Of those that a mesh axis runs over, the one named last changes fastest.
Arguments:
- grid_fields: bfloat16 [4, 64, 512, 1024], P('member', 'lev', 'wave'), parts along dimension 0, may hold values from -6 to 6
- band_latitude: int32 [512], replicated, may hold values from 0 to 511, as said below
- wave_of_slot: int32 [512], replicated, may hold values from 0 to 511, as said below
- legendre: bfloat16 [512, 2, 256, 256], P('wave'), may hold values from -0.25 to 0.25
- quad_weight: float32 [256], replicated, may hold values from 0.5 to 1.5
- wave_speed: float32 [128], P('member'), parts along dimension 0, may hold values from 0.5 to 4
- layer_depth: float32 [128], P('member'), parts along dimension 0, may hold values from 0.25 to 2
- diffusion: float32 [128], P('member'), parts along dimension 0, may hold values from 0.5 to 8
Outputs:
- grid_out: bfloat16 [4, 64, 512, 1024], P('member', 'lev', 'wave'), parts along dimension 0
The draws below stay inside these ranges and needn't reach their ends.
There are 2 independent parts, one for each index of `member`. The reference program is written for one: setup_inputs(seed, part) draws one part's arguments, and reference() takes and returns one part's arrays. A program takes and returns all parts, laid end to end along the dimension named above; an argument that names none is the same for every part. Nothing has to cross between parts.
Inputs may be any that keep to these rules, and one draw needn't show every extreme that they name: `wave_of_slot`: A permutation of the 512 wavenumbers in which slots 2 k and 2 k + 1 hold a wavenumber m < 256 and 511 - m. `band_latitude`: A permutation of the 512 latitudes; each aligned block of 128 rows holds 64 latitudes i < 256 followed by their mirrors 512 - 1 - i in the same order.
All inputs are finite; a program needn't handle non-finite values.
Results may differ from the reference program's by a relative error of at most 0.017.
Values may be sent and summed in bfloat16 or wider, within the bound.
No kernel may reach another device: no remote copies, remote signals or barrier semaphores. Data moves between devices by JAX's collectives and lax.ppermute only.
A program may use at most 192 MiB of HBM per device.

```python
import math
import jax
import jax.numpy as jnp
from jax import lax

NLON = 1024
NLAT = 512
MW = 512
FIELDS = 2
LEVELS = 64
LAT_DEV = 128


def draw_wave_of_slot(key, part):
    lower = jax.random.permutation(jax.random.fold_in(key, 11), MW // 2).astype(jnp.int32)
    return jnp.stack([lower, MW - 1 - lower], axis=1).reshape(MW)


def draw_band_latitude(key, part):
    northern = jax.random.permutation(jax.random.fold_in(key, 12), NLAT // 2).astype(jnp.int32)
    northern = northern.reshape(NLAT // LAT_DEV, LAT_DEV // 2)
    return jnp.concatenate([northern, NLAT - 1 - northern], axis=1).reshape(NLAT)


def levels(rng, dims, cuts, least, largest):
    loudness, own = 1.0, jax.random.fold_in(rng, 6)
    for axis_at, parts in cuts:
        draws = jnp.exp(jax.random.uniform(jax.random.fold_in(own, axis_at), (parts,), jnp.float32, least / len(cuts), largest / len(cuts)))
        loudness = loudness * jnp.repeat(draws, dims[axis_at] // parts).reshape([-1 if axis == axis_at else 1 for axis in range(len(dims))])
    return loudness


def bell_draw(own_key, dims, spread, reach, shards=(), kind=jnp.bfloat16):
    drawn = jax.random.normal(own_key, dims, jnp.float32) * spread
    if len(shards) > 0:
        drawn = levels(own_key, dims, shards, -0.22, 0.18) * drawn
    return jnp.clip(drawn, min=-reach, max=reach).astype(kind)


def setup_inputs(seed: int = 0, part: int = 0) -> dict:
    key_list = jax.random.split(jax.random.key(seed), 9)
    own_keys = jax.random.split(jax.random.fold_in(key_list[8], part), 9)
    return {
        "grid_fields": bell_draw(own_keys[0], (FIELDS, LEVELS, NLAT, NLON), 1.0, 6.0, ((1, 4), (2, 4))),
        "band_latitude": draw_band_latitude(jax.random.fold_in(key_list[8], 71), part),
        "wave_of_slot": draw_wave_of_slot(jax.random.fold_in(key_list[8], 71), part),
        "legendre": bell_draw(key_list[3], (MW, 2, NLAT // 2, MW // 2), NLAT ** -0.5, 0.25, ((0, 4),)),
        "quad_weight": jnp.clip(jax.random.uniform(key_list[4], (NLAT // 2,), jnp.float32, 0.5, 1.5), 0.5, 1.5),
        "wave_speed": jnp.clip(jnp.exp(jax.random.uniform(own_keys[5], (LEVELS,), jnp.float32, math.log(0.5), math.log(4.0))), 0.5, 4.0),
        "layer_depth": jnp.clip(jnp.exp(jax.random.uniform(own_keys[6], (LEVELS,), jnp.float32, math.log(0.25), math.log(2.0))), 0.25, 2.0),
        "diffusion": jnp.clip(jnp.exp(jax.random.uniform(own_keys[7], (LEVELS,), jnp.float32, math.log(0.5), math.log(8.0))), 0.5, 8.0),
    }


def dynamics(spectrum, degree, wave_speed, layer_depth, diffusion):
    eigen_value = (degree * (degree + 1)).astype(jnp.float32) / float(MW * (MW - 1))
    eigen_value = eigen_value[None, :, None, :]
    speed_col = wave_speed[:, None, None, None]
    depth_col = layer_depth[:, None, None, None]
    diffusion_col = diffusion[:, None, None, None]
    divergence = spectrum[0]
    geopotential = spectrum[1]
    new_div = (divergence + speed_col * eigen_value * geopotential) / (1.0 + speed_col * depth_col * eigen_value)
    new_geo = geopotential - depth_col * new_div
    damping = jnp.where(degree[None, :, None, :] < MW, 1.0 / (1.0 + diffusion_col * eigen_value * eigen_value), 0.0)
    return jnp.stack([new_div * damping, new_geo * damping]).astype(jnp.bfloat16)

def reference(grid_fields, band_latitude, wave_of_slot, legendre, quad_weight, wave_speed, layer_depth, diffusion):
    north_count = NLAT // 2
    scaling = math.sqrt(2.0 / NLON)
    positions = jnp.arange(NLAT, dtype=jnp.int32)
    row_of_lat = jnp.zeros((NLAT,), jnp.int32).at[band_latitude].set(positions)
    north_rows = row_of_lat[:north_count]
    south_rows = row_of_lat[NLAT - 1 - jnp.arange(north_count, dtype=jnp.int32)]
    coeff_list = []
    for field_index in range(FIELDS):
        spectrum = jnp.fft.rfft(grid_fields[field_index].astype(jnp.float32), axis=-1)[..., wave_of_slot]
        parts_pair = jnp.stack([jnp.real(spectrum), jnp.imag(spectrum)], axis=-1) * scaling
        coeff_list.append(parts_pair.astype(jnp.bfloat16))
    fourier = jnp.stack(coeff_list)
    northern = fourier[:, :, north_rows].astype(jnp.float32)
    southern = fourier[:, :, south_rows].astype(jnp.float32)
    weights = quad_weight[:, None, None]
    symmetric = ((northern + southern) * weights).astype(jnp.bfloat16)
    antisymmetric = ((northern - southern) * weights).astype(jnp.bfloat16)
    legendre_full = legendre.astype(jnp.float32)
    columns = jnp.arange(MW // 2, dtype=jnp.int32)
    inverse_parts = []
    for parity, source in ((0, symmetric), (1, antisymmetric)):
        table_part = legendre_full[:, parity]
        spectral = jnp.einsum('flhsc,shj->flscj', source.astype(jnp.float32), table_part, precision=lax.Precision.HIGHEST)
        degree = wave_of_slot[:, None] + 2 * columns[None, :] + parity
        stepped = dynamics(spectral, degree, wave_speed, layer_depth, diffusion)
        inverse_parts.append(jnp.einsum('flscj,shj->flhsc', stepped.astype(jnp.float32), table_part, precision=lax.Precision.HIGHEST))
    even_part, odd_part = inverse_parts
    northern_out = (even_part + odd_part).astype(jnp.bfloat16)
    southern_out = (even_part - odd_part).astype(jnp.bfloat16)
    by_latitude = jnp.concatenate([northern_out, southern_out[:, :, ::-1]], axis=2)
    back = by_latitude[:, :, band_latitude].astype(jnp.float32)
    complex_part = back[..., 0] + 1j * back[..., 1]
    factors = jnp.where(wave_of_slot == 0, float(NLON), float(NLON // 2))
    full_spectrum = jnp.zeros(back.shape[:3] + (NLON // 2 + 1,), complex_part.dtype)
    full_spectrum = full_spectrum.at[..., wave_of_slot].set(complex_part * factors)
    grid = jnp.fft.irfft(full_spectrum, n=NLON, axis=-1) * scaling
    return grid.astype(jnp.bfloat16)
```

```python
import math

import jax
import jax.numpy as jnp
from jax import lax
from jax.experimental import pallas as pl
from jax.experimental.pallas import tpu as pltpu
from jax.sharding import PartitionSpec as P

LANES = 128
BF16 = jnp.bfloat16
F32 = jnp.float32


def params(semantics, vmem_mb=56):
    return pltpu.CompilerParams(
        dimension_semantics=semantics, vmem_limit_bytes=vmem_mb * 1024 * 1024
    )


def wave_table(wave_col, shift_col, lon_count):
    rows = wave_col.shape[0]
    scaling = math.sqrt(2.0 / lon_count)
    quarter = lon_count // 4

    def body(m_ref, shift_ref, out_ref):
        m = m_ref[...]
        shift = shift_ref[...]
        lane = lax.broadcasted_iota(jnp.int32, (rows, LANES), 1)

        def turn(phase):
            wrapped = jnp.bitwise_and(phase, lon_count - 1)
            centred = jnp.where(wrapped >= lon_count // 2, wrapped - lon_count, wrapped)
            return jnp.cos(centred.astype(F32) * (2.0 * math.pi / lon_count))

        fine = m * lane
        coarse = m * (lane * LANES) + shift
        fine_cos = turn(fine)
        fine_sin = turn(fine - quarter)
        coarse_cos = turn(coarse) * scaling
        coarse_sin = turn(coarse - quarter) * scaling
        for a in range(lon_count // LANES):
            piece = coarse_cos[:, a : a + 1] * fine_cos - coarse_sin[:, a : a + 1] * fine_sin
            out_ref[:, a * LANES : (a + 1) * LANES] = piece.astype(BF16)

    return pl.pallas_call(
        body,
        out_shape=jax.ShapeDtypeStruct((rows, lon_count), BF16),
        cost_estimate=pl.CostEstimate(
            flops=rows * lon_count * 8, bytes_accessed=rows * lon_count * 2, transcendentals=0
        ),
        name="wave_table",
    )(wave_col, shift_col)


def forward_fourier(grid_rows, weight_col, table, after, peers):
    merged, _, half, lon_count = grid_rows.shape
    lat_dev = 2 * half
    rows = table.shape[0]
    part = rows // peers
    step = max(1, min(merged, 512 // lat_dev))

    def body(g_ref, w_ref, t_ref, *rest):
        outs = rest[len(after) :]
        g = g_ref[...].astype(F32)
        w = w_ref[...]
        north, south = g[:, 0], g[:, 1]
        sym = ((north + south) * w).astype(BF16)
        anti = ((north - south) * w).astype(BF16)
        both = jnp.concatenate([sym, anti], axis=1).reshape(step * lat_dev, lon_count)
        acc = lax.dot_general(
            t_ref[...], both, (((1,), (1,)), ((), ())), preferred_element_type=F32
        )
        for d in range(peers):
            outs[d][...] = acc[d * part : (d + 1) * part].astype(BF16)

    return pl.pallas_call(
        body,
        grid=(merged // step,),
        in_specs=[
            pl.BlockSpec((step, 2, half, lon_count), lambda i: (i, 0, 0, 0)),
            pl.BlockSpec((half, 1), lambda i: (0, 0)),
            pl.BlockSpec((rows, lon_count), lambda i: (0, 0)),
        ]
        + [pl.BlockSpec(memory_space=pl.ANY) for _ in after],
        out_specs=[pl.BlockSpec((part, step * lat_dev), lambda i: (0, i)) for _ in range(peers)],
        out_shape=[jax.ShapeDtypeStruct((part, merged * lat_dev), BF16) for _ in range(peers)],
        compiler_params=params(("arbitrary",)),
        cost_estimate=pl.CostEstimate(
            flops=2 * rows * lon_count * merged * lat_dev,
            bytes_accessed=2 * merged * lat_dev * (lon_count + rows),
            transcendentals=0,
        ),
        name="forward_fourier",
    )(grid_rows, weight_col, table, *after)


def legendre_stage(pieces, legendre, chunk, wave_rows, gather, scatter, level_cols, wave_count):
    peers = len(pieces)
    _, slots, merged, lat_dev = pieces[0].shape
    lat_count, width = legendre.shape[2:]
    levels = level_cols[0].shape[0]
    step = math.gcd(slots, 4)
    aligned = lat_dev % LANES == 0
    rows = 2 * merged
    inverse_norm = float(wave_count * (wave_count - 1))

    def body(m_ref, *refs):
        ins = refs[:peers]
        table_ref, gather_ref, scatter_ref, a_ref, b_ref, k_ref = refs[peers : peers + 6]
        outs = refs[peers + 6 :]
        flat = [r[...].reshape(2 * step * merged, lat_dev) for r in ins]
        if aligned:
            ordered = lax.dot_general(
                jnp.concatenate(flat, axis=1),
                gather_ref[...],
                (((1,), (0,)), ((), ())),
                preferred_element_type=F32,
            )
        else:
            ordered = 0.0
            for d in range(peers):
                ordered = ordered + lax.dot_general(
                    flat[d],
                    gather_ref[d * lat_dev : (d + 1) * lat_dev, :],
                    (((1,), (0,)), ((), ())),
                    preferred_element_type=F32,
                )
        ordered = ordered.astype(BF16).reshape(2, step, merged, 2 * lat_count)
        speed, depth, diff = a_ref[...], b_ref[...], k_ref[...]
        speed_depth = speed * depth
        column = lax.broadcasted_iota(jnp.int32, (1, width), 1)
        results = []
        for s in range(step):
            wave = m_ref[pl.program_id(0) * step + s]
            halves = []
            for parity in range(2):
                source = ordered[:, s, :, parity * lat_count : (parity + 1) * lat_count]
                source = source.reshape(rows, lat_count)
                spec = lax.dot_general(
                    source,
                    table_ref[s, parity],
                    (((1,), (0,)), ((), ())),
                    preferred_element_type=F32,
                )
                spec = spec.reshape(2, 2, levels, width)
                degree = wave + 2 * column + parity
                eigen = (degree * (degree + 1)).astype(F32) / inverse_norm
                damp = jnp.where(
                    degree < wave_count, 1.0 / (1.0 + diff * (eigen * eigen)), 0.0
                )
                implicit = 1.0 / (1.0 + speed_depth * eigen)
                coupling = speed * eigen
                stepped = []
                for c in range(2):
                    geo = spec[c, 1]
                    new_div = (spec[c, 0] + coupling * geo) * implicit
                    new_geo = geo - depth * new_div
                    stepped.append((new_div * damp).astype(BF16))
                    stepped.append((new_geo * damp).astype(BF16))
                halves.append(
                    lax.dot_general(
                        jnp.concatenate(stepped, axis=0),
                        table_ref[s, parity],
                        (((1,), (1,)), ((), ())),
                        preferred_element_type=F32,
                    ).astype(BF16)
                )
            results.append(jnp.concatenate(halves, axis=1))
        joined = jnp.concatenate(results, axis=0)
        if aligned:
            spread = lax.dot_general(
                joined, scatter_ref[...], (((1,), (0,)), ((), ())), preferred_element_type=F32
            ).astype(BF16)
        for d in range(peers):
            span = slice(d * lat_dev, (d + 1) * lat_dev)
            if aligned:
                piece = spread[:, span]
            else:
                piece = lax.dot_general(
                    joined,
                    scatter_ref[:, span],
                    (((1,), (0,)), ((), ())),
                    preferred_element_type=F32,
                ).astype(BF16)
            piece = piece.reshape(step, 2, merged, lat_dev)
            for c in range(2):
                outs[d][c] = piece[:, c]

    steps = slots // step
    piece_spec = pl.BlockSpec((2, step, merged, lat_dev), lambda i, m: (0, i, 0, 0))
    whole = lambda i, m: (0, 0)
    full = 2 * lat_count
    return pl.pallas_call(
        body,
        grid_spec=pltpu.PrefetchScalarGridSpec(
            num_scalar_prefetch=1,
            grid=(steps,),
            in_specs=[piece_spec] * peers
            + [
                pl.BlockSpec(
                    (step, 2, lat_count, width), lambda i, m: (chunk * steps + i, 0, 0, 0)
                ),
                pl.BlockSpec((full, full), whole),
                pl.BlockSpec((full, full), whole),
            ]
            + [pl.BlockSpec((levels, 1), whole)] * 3,
            out_specs=[piece_spec] * peers,
        ),
        out_shape=[jax.ShapeDtypeStruct(pieces[0].shape, BF16) for _ in range(peers)],
        compiler_params=params(("arbitrary",)),
        cost_estimate=pl.CostEstimate(
            flops=16 * slots * rows * lat_count * width,
            bytes_accessed=slots * (4 * lat_count * width + 8 * rows * lat_count),
            transcendentals=0,
        ),
        name="legendre_stage",
    )(wave_rows, *pieces, legendre, gather, scatter, *level_cols)


def inverse_fourier(pieces, tables, merged, lat_dev):
    part = pieces[0].shape[0]
    count = len(pieces)
    lon_count = tables[0].shape[1]
    half = lat_dev // 2
    step = max(1, min(merged, 512 // lat_dev))

    def body(*refs):
        ins, ts, out_ref = refs[:count], refs[count:-1], refs[-1]
        spectrum = jnp.concatenate([r[...] for r in ins], axis=0)
        table = jnp.concatenate([t[...] for t in ts], axis=0)
        acc = lax.dot_general(
            spectrum, table, (((0,), (0,)), ((), ())), preferred_element_type=F32
        )
        acc = acc.reshape(step, 2, half, lon_count)
        even, odd = acc[:, 0], acc[:, 1]
        out_ref[:, 0] = (even + odd).astype(BF16)
        out_ref[:, 1] = (even - odd).astype(BF16)

    return pl.pallas_call(
        body,
        grid=(merged // step,),
        in_specs=[pl.BlockSpec((part, step * lat_dev), lambda i: (0, i)) for _ in pieces]
        + [pl.BlockSpec(t.shape, lambda i: (0, 0)) for t in tables],
        out_specs=pl.BlockSpec((step, 2, half, lon_count), lambda i: (i, 0, 0, 0)),
        out_shape=jax.ShapeDtypeStruct((merged, 2, half, lon_count), BF16),
        compiler_params=params(("arbitrary",)),
        cost_estimate=pl.CostEstimate(
            flops=2 * part * count * lon_count * merged * lat_dev,
            bytes_accessed=2 * merged * lat_dev * (lon_count + part * count),
            transcendentals=0,
        ),
        name="inverse_fourier",
    )(*pieces, *tables)


def per_device(
    grid_fields,
    band_latitude,
    wave_of_slot,
    legendre,
    quad_weight,
    wave_speed,
    layer_depth,
    diffusion,
    peers,
):
    fields, levels, lat_dev, lon_count = grid_fields.shape
    wave_count = wave_of_slot.shape[0]
    lat_count = quad_weight.shape[0]
    half = lat_dev // 2
    merged = fields * levels
    slot_count = legendre.shape[0]
    chunks = math.gcd(slot_count // math.gcd(slot_count, 8), 4)
    slots = slot_count // chunks
    me = lax.axis_index("wave")
    paired = peers & (peers - 1) == 0
    offsets = jnp.arange(peers, dtype=jnp.int32)
    target = me ^ offsets if paired else (me + offsets) % peers
    origin = target if paired else (me - offsets) % peers

    def swap(values, d, back):
        if d == 0:
            return values
        if paired:
            pairs = [(i, i ^ d) for i in range(peers)]
        elif back:
            pairs = [(i, (i - d) % peers) for i in range(peers)]
        else:
            pairs = [(i, (i + d) % peers) for i in range(peers)]
        return lax.ppermute(values, "wave", pairs)

    def pick(values, index):
        hit = index[:, None] == offsets[None, :]
        return jnp.sum(jnp.where(hit[:, :, None], values[None], 0), axis=1)

    waves = pick(wave_of_slot.reshape(peers, slot_count), target)
    waves = waves.reshape(peers, chunks, 1, slots)
    shift = jnp.arange(2, dtype=jnp.int32)[:, None] * (lon_count // 4)
    mine = waves[0, :, 0, :]
    lat_north = band_latitude.reshape(peers, 2, half)[:, 0, :]
    lat_origin = pick(lat_north, origin)
    parity_lat = lat_origin[:, None, :] + jnp.array([0, lat_count], jnp.int32)[None, :, None]
    parity_lat = parity_lat.reshape(peers * lat_dev)
    every = jnp.arange(2 * lat_count, dtype=jnp.int32)
    gather = (parity_lat[:, None] == every[None, :]).astype(BF16)
    scatter = (every[:, None] == parity_lat[None, :]).astype(BF16)
    local_hit = lat_origin[0][:, None] == jnp.arange(lat_count, dtype=jnp.int32)[None, :]
    weight_col = jnp.sum(jnp.where(local_hit, quad_weight[None, :], 0.0), axis=1, keepdims=True)
    level_start = lax.axis_index("lev") * levels
    level_cols = [
        lax.dynamic_slice_in_dim(v, level_start, levels, 0)[:, None]
        for v in (wave_speed, layer_depth, diffusion)
    ]
    grid_rows = grid_fields.reshape(merged, 2, half, lon_count)
    table_rows = peers * 2 * slots
    tables, received = [], []
    sent_back = []
    for k in range(chunks):
        wave_k = jnp.broadcast_to(waves[:, k], (peers, 2, slots)).reshape(table_rows, 1)
        shift_k = jnp.broadcast_to(shift[None], (peers, 2, slots)).reshape(table_rows, 1)
        table = wave_table(wave_k, shift_k, lon_count)
        tables.append(table)
        after = received[k - 2][1:] if k >= 2 else []
        blocks = forward_fourier(grid_rows, weight_col, table, after, peers)
        received.append([swap(b, d, False) for d, b in enumerate(blocks)])
    for k in range(chunks):
        pieces = [r.reshape(2, slots, merged, lat_dev) for r in received[k]]
        outs = legendre_stage(
            pieces, legendre, k, mine[k], gather, scatter, level_cols, wave_count
        )
        outs = [o.reshape(2 * slots, merged * lat_dev) for o in outs]
        sent_back += [swap(o, d, True) for d, o in enumerate(outs)]
    grid_out = inverse_fourier(sent_back, tables, merged, lat_dev)
    return grid_out.reshape(fields, levels, lat_dev, lon_count)


def solution(mesh):
    peers = mesh.shape["wave"]

    def body(*args):
        return per_device(*args, peers=peers)

    in_specs = (
        P("member", "lev", "wave", None),
        P(),
        P(),
        P("wave", None, None, None),
        P(),
        P("member"),
        P("member"),
        P("member"),
    )
    out_specs = P("member", "lev", "wave", None)
    return jax.shard_map(
        body, mesh=mesh, in_specs=in_specs, out_specs=out_specs, check_vma=False
    )
```

```python
import math

import jax
import jax.numpy as jnp
from jax import lax
from jax.experimental import pallas as pl
from jax.experimental.pallas import tpu as pltpu
from jax.sharding import PartitionSpec as P

LANES = 128
BF16 = jnp.bfloat16
F32 = jnp.float32


def params(semantics, vmem_mb=56):
    return pltpu.CompilerParams(
        dimension_semantics=semantics, vmem_limit_bytes=vmem_mb * 1024 * 1024
    )


def wave_table(wave_row, band_row, weight_row, me, chunk, slots, lon_count, half, peers, paired, after):
    slot_count = wave_row.shape[1] // peers
    lat_dev = 2 * half
    pairs = peers * slots
    scaling = math.sqrt(2.0 / lon_count)
    root = math.sqrt(0.5)

    def body(me_ref, wave_ref, band_ref, weight_ref, *rest):
        out_ref, w_ref = rest[len(after) :]
        here = me_ref[0]
        spot = lax.broadcasted_iota(jnp.int32, (pairs, wave_row.shape[1]), 1)
        row = lax.broadcasted_iota(jnp.int32, (pairs, wave_row.shape[1]), 0)
        offset = row // slots
        owner = jnp.bitwise_xor(offset, here) if paired else (offset + here) % peers
        slot = owner * slot_count + chunk * slots + (row - offset * slots)
        wave = jnp.where(spot == slot, wave_ref[...].astype(F32), 0.0)
        m = jnp.sum(wave, axis=1, keepdims=True).astype(jnp.int32)
        lane = lax.broadcasted_iota(jnp.int32, (pairs, LANES), 1)
        wrapped = jnp.bitwise_and(m * lane, lon_count - 1)
        centred = jnp.where(wrapped >= lon_count // 2, wrapped - lon_count, wrapped)
        angle = centred.astype(F32) * (2.0 * math.pi / lon_count)
        fine_cos = jnp.cos(angle) * scaling
        fine_sin = jnp.sin(angle) * scaling
        for a in range(lon_count // LANES):
            turn = jnp.bitwise_and(m * (a * LANES), lon_count - 1).astype(F32)
            turn = turn * (2.0 * math.pi / lon_count)
            coarse_cos = jnp.broadcast_to(jnp.cos(turn), (pairs, LANES))
            coarse_sin = jnp.broadcast_to(jnp.sin(turn), (pairs, LANES))
            cos = (coarse_cos * fine_cos - coarse_sin * fine_sin).astype(BF16)
            sin = (-coarse_sin * fine_cos - coarse_cos * fine_sin).astype(BF16)
            span = slice(a * LANES, (a + 1) * LANES)
            for d in range(peers):
                top = 2 * d * slots
                out_ref[top : top + slots, span] = cos[d * slots : (d + 1) * slots]
                out_ref[top + slots : top + 2 * slots, span] = sin[d * slots : (d + 1) * slots]
        place = lax.broadcasted_iota(jnp.int32, (half, band_row.shape[1]), 1)
        local = lax.broadcasted_iota(jnp.int32, (half, band_row.shape[1]), 0) + here * lat_dev
        lat = jnp.where(place == local, band_ref[...].astype(F32), 0.0)
        lat = jnp.sum(lat, axis=1, keepdims=True).astype(jnp.int32)
        north = lax.broadcasted_iota(jnp.int32, (half, weight_row.shape[1]), 1)
        w_ref[...] = jnp.sum(
            jnp.where(north == lat, weight_ref[...], 0.0), axis=1, keepdims=True
        )

    rows = 2 * pairs
    vmem = pl.BlockSpec(memory_space=pltpu.VMEM)
    return pl.pallas_call(
        body,
        in_specs=[pl.BlockSpec(memory_space=pltpu.SMEM), vmem, vmem, vmem]
        + [pl.BlockSpec(memory_space=pl.ANY) for _ in after],
        out_shape=[
            jax.ShapeDtypeStruct((rows, lon_count), BF16),
            jax.ShapeDtypeStruct((half, 1), F32),
        ],
        cost_estimate=pl.CostEstimate(
            flops=rows * lon_count * 8, bytes_accessed=rows * lon_count * 2, transcendentals=0
        ),
        name="wave_table",
    )(me, wave_row, band_row, weight_row, *after)


def row_step(merged, lat_dev, split):
    return math.gcd(merged // split, max(1, 512 // lat_dev))


def forward_fourier(grid_rows, weight_col, table, peers, split, index):
    merged, _, half, lon_count = grid_rows.shape
    lat_dev = 2 * half
    rows = table.shape[0]
    part = rows // peers
    step = row_step(merged, lat_dev, split)
    steps = merged // split // step

    def body(g_ref, w_ref, t_ref, *outs):
        g = g_ref[...].astype(F32)
        w = w_ref[...]
        north, south = g[:, 0], g[:, 1]
        sym = ((north + south) * w).astype(BF16)
        anti = ((north - south) * w).astype(BF16)
        both = jnp.concatenate([sym, anti], axis=1).reshape(step * lat_dev, lon_count)
        acc = lax.dot_general(
            t_ref[...], both, (((1,), (1,)), ((), ())), preferred_element_type=F32
        )
        for d in range(peers):
            outs[d][...] = acc[d * part : (d + 1) * part].astype(BF16)

    count = merged // split * lat_dev
    return pl.pallas_call(
        body,
        grid=(steps,),
        in_specs=[
            pl.BlockSpec((step, 2, half, lon_count), lambda i: (i + index * steps, 0, 0, 0)),
            pl.BlockSpec((half, 1), lambda i: (0, 0)),
            pl.BlockSpec((rows, lon_count), lambda i: (0, 0)),
        ],
        out_specs=[pl.BlockSpec((part, step * lat_dev), lambda i: (0, i)) for _ in range(peers)],
        out_shape=[jax.ShapeDtypeStruct((part, count), BF16) for _ in range(peers)],
        compiler_params=params(("arbitrary",)),
        cost_estimate=pl.CostEstimate(
            flops=2 * rows * lon_count * count,
            bytes_accessed=2 * count * (lon_count + rows),
            transcendentals=0,
        ),
        name="forward_fourier",
    )(grid_rows, weight_col, table)


def legendre_stage(pieces, legendre, chunk, wave_rows, gather, scatter, level_cols, wave_count):
    peers = len(pieces)
    _, slots, merged, lat_dev = pieces[0].shape
    lat_count, width = legendre.shape[2:]
    levels = level_cols[0].shape[0]
    step = math.gcd(slots, 4)
    aligned = lat_dev % LANES == 0
    rows = 2 * merged
    inverse_norm = float(wave_count * (wave_count - 1))

    def body(m_ref, *refs):
        ins = refs[:peers]
        table_ref, gather_ref, scatter_ref, a_ref, b_ref, k_ref = refs[peers : peers + 6]
        outs = refs[peers + 6 :]
        flat = [r[...].reshape(2 * step * merged, lat_dev) for r in ins]
        if aligned:
            ordered = lax.dot_general(
                jnp.concatenate(flat, axis=1),
                gather_ref[...],
                (((1,), (0,)), ((), ())),
                preferred_element_type=F32,
            )
        else:
            ordered = 0.0
            for d in range(peers):
                ordered = ordered + lax.dot_general(
                    flat[d],
                    gather_ref[d * lat_dev : (d + 1) * lat_dev, :],
                    (((1,), (0,)), ((), ())),
                    preferred_element_type=F32,
                )
        ordered = ordered.astype(BF16).reshape(2, step, merged, 2 * lat_count)
        speed, depth, diff = a_ref[...], b_ref[...], k_ref[...]
        speed_depth = speed * depth
        column = lax.broadcasted_iota(jnp.int32, (1, width), 1)
        results = []
        for s in range(step):
            wave = m_ref[pl.program_id(0) * step + s]
            halves = []
            for parity in range(2):
                source = ordered[:, s, :, parity * lat_count : (parity + 1) * lat_count]
                source = source.reshape(rows, lat_count)
                spec = lax.dot_general(
                    source,
                    table_ref[s, parity],
                    (((1,), (0,)), ((), ())),
                    preferred_element_type=F32,
                )
                spec = spec.reshape(2, 2, levels, width)
                degree = wave + 2 * column + parity
                eigen = (degree * (degree + 1)).astype(F32) / inverse_norm
                damp = jnp.where(
                    degree < wave_count, 1.0 / (1.0 + diff * (eigen * eigen)), 0.0
                )
                implicit = 1.0 / (1.0 + speed_depth * eigen)
                coupling = speed * eigen
                stepped = []
                for c in range(2):
                    geo = spec[c, 1]
                    new_div = (spec[c, 0] + coupling * geo) * implicit
                    new_geo = geo - depth * new_div
                    stepped.append((new_div * damp).astype(BF16))
                    stepped.append((new_geo * damp).astype(BF16))
                halves.append(
                    lax.dot_general(
                        jnp.concatenate(stepped, axis=0),
                        table_ref[s, parity],
                        (((1,), (1,)), ((), ())),
                        preferred_element_type=F32,
                    ).astype(BF16)
                )
            results.append(jnp.concatenate(halves, axis=1))
        joined = jnp.concatenate(results, axis=0)
        if aligned:
            spread = lax.dot_general(
                joined, scatter_ref[...], (((1,), (0,)), ((), ())), preferred_element_type=F32
            ).astype(BF16)
        for d in range(peers):
            span = slice(d * lat_dev, (d + 1) * lat_dev)
            if aligned:
                piece = spread[:, span]
            else:
                piece = lax.dot_general(
                    joined,
                    scatter_ref[:, span],
                    (((1,), (0,)), ((), ())),
                    preferred_element_type=F32,
                ).astype(BF16)
            piece = piece.reshape(step, 2, merged, lat_dev)
            for c in range(2):
                outs[d][c] = piece[:, c]

    steps = slots // step
    piece_spec = pl.BlockSpec((2, step, merged, lat_dev), lambda i, m: (0, i, 0, 0))
    whole = lambda i, m: (0, 0)
    full = 2 * lat_count
    return pl.pallas_call(
        body,
        grid_spec=pltpu.PrefetchScalarGridSpec(
            num_scalar_prefetch=1,
            grid=(steps,),
            in_specs=[piece_spec] * peers
            + [
                pl.BlockSpec(
                    (step, 2, lat_count, width), lambda i, m: (chunk * steps + i, 0, 0, 0)
                ),
                pl.BlockSpec((full, full), whole),
                pl.BlockSpec((full, full), whole),
            ]
            + [pl.BlockSpec((levels, 1), whole)] * 3,
            out_specs=[piece_spec] * peers,
        ),
        out_shape=[jax.ShapeDtypeStruct(pieces[0].shape, BF16) for _ in range(peers)],
        compiler_params=params(("arbitrary",)),
        cost_estimate=pl.CostEstimate(
            flops=16 * slots * rows * lat_count * width,
            bytes_accessed=slots * (4 * lat_count * width + 8 * rows * lat_count),
            transcendentals=0,
        ),
        name="legendre_stage",
    )(wave_rows, *pieces, legendre, gather, scatter, *level_cols)


def inverse_fourier(pieces, table, merged, lat_dev, split, index, previous):
    part = pieces[0].shape[0]
    count = len(pieces)
    lon_count = table.shape[1]
    half = lat_dev // 2
    step = row_step(merged, lat_dev, split)
    steps = merged // split // step

    def body(*refs):
        ins, table_ref, out_ref = refs[:count], refs[count], refs[-1]
        spectrum = jnp.concatenate([r[...] for r in ins], axis=0)
        acc = lax.dot_general(
            spectrum, table_ref[...], (((0,), (0,)), ((), ())), preferred_element_type=F32
        )
        acc = acc.reshape(step, 2, half, lon_count)
        even, odd = acc[:, 0], acc[:, 1]
        out_ref[:, 0] = (even + odd).astype(BF16)
        out_ref[:, 1] = (even - odd).astype(BF16)

    def piece_spec(piece):
        start = index * steps if piece.shape[1] == merged * lat_dev else 0
        return pl.BlockSpec((part, step * lat_dev), lambda i: (0, i + start))

    earlier = [] if previous is None else [previous]
    return pl.pallas_call(
        body,
        grid=(steps,),
        in_specs=[piece_spec(p) for p in pieces]
        + [pl.BlockSpec(table.shape, lambda i: (0, 0))]
        + [pl.BlockSpec(memory_space=pl.ANY) for _ in earlier],
        out_specs=pl.BlockSpec((step, 2, half, lon_count), lambda i: (i + index * steps, 0, 0, 0)),
        out_shape=jax.ShapeDtypeStruct((merged, 2, half, lon_count), BF16),
        input_output_aliases={count + 1: 0} if earlier else {},
        compiler_params=params(("arbitrary",)),
        cost_estimate=pl.CostEstimate(
            flops=2 * part * count * lon_count * merged * lat_dev // split,
            bytes_accessed=2 * merged * lat_dev * (lon_count + part * count) // split,
            transcendentals=0,
        ),
        name="inverse_fourier",
    )(*pieces, table, *earlier)


def per_device(
    grid_fields,
    band_latitude,
    wave_of_slot,
    legendre,
    quad_weight,
    wave_speed,
    layer_depth,
    diffusion,
    peers,
):
    fields, levels, lat_dev, lon_count = grid_fields.shape
    wave_count = wave_of_slot.shape[0]
    lat_count = quad_weight.shape[0]
    half = lat_dev // 2
    merged = fields * levels
    slot_count = legendre.shape[0]
    chunks = math.gcd(slot_count // math.gcd(slot_count, 8), 4)
    slots = slot_count // chunks
    me = lax.axis_index("wave")
    paired = peers & (peers - 1) == 0
    offsets = jnp.arange(peers, dtype=jnp.int32)
    origin = me ^ offsets if paired else (me - offsets) % peers

    def swap(values, d, back):
        if d == 0:
            return values
        if paired:
            pairs = [(i, i ^ d) for i in range(peers)]
        elif back:
            pairs = [(i, (i - d) % peers) for i in range(peers)]
        else:
            pairs = [(i, (i + d) % peers) for i in range(peers)]
        return lax.ppermute(values, "wave", pairs)

    def pick(values, index):
        hit = index[:, None] == offsets[None, :]
        return jnp.sum(jnp.where(hit[:, :, None], values[None], 0), axis=1)

    mine = lax.dynamic_slice_in_dim(wave_of_slot, me * slot_count, slot_count, 0)
    lat_north = band_latitude.reshape(peers, 2, half)[:, 0, :]
    lat_origin = pick(lat_north, origin)
    parity_lat = lat_origin[:, None, :] + jnp.array([0, lat_count], jnp.int32)[None, :, None]
    parity_lat = parity_lat.reshape(peers * lat_dev)
    every = jnp.arange(2 * lat_count, dtype=jnp.int32)
    gather = (parity_lat[:, None] == every[None, :]).astype(BF16)
    scatter = (every[:, None] == parity_lat[None, :]).astype(BF16)
    level_start = lax.axis_index("lev") * levels
    level_cols = [
        lax.dynamic_slice_in_dim(v, level_start, levels, 0)[:, None]
        for v in (wave_speed, layer_depth, diffusion)
    ]
    grid_rows = grid_fields.reshape(merged, 2, half, lon_count)
    wave_row, band_row, weight_row = (
        v.reshape(1, -1) for v in (wave_of_slot, band_latitude, quad_weight)
    )
    me_cell = me.astype(jnp.int32).reshape(1)
    first_split = math.gcd(merged, 2)
    last_split = math.gcd(merged, 4)
    while merged // last_split * lat_dev % LANES:
        last_split //= 2
    tables, received = [], []
    blocks = []
    for k in range(chunks):
        table, local_weight = wave_table(
            wave_row,
            band_row,
            weight_row,
            me_cell,
            k,
            slots,
            lon_count,
            half,
            peers,
            paired,
            blocks[:1],
        )
        weight_col = local_weight if k == 0 else weight_col
        tables.append(table)
        split = first_split if k == 0 else 1
        shape = (2, slots, merged // split, lat_dev)
        parts = []
        for h in range(split):
            blocks = forward_fourier(grid_rows, weight_col, table, peers, split, h)
            parts.append([swap(b, d, False).reshape(shape) for d, b in enumerate(blocks)])
        received.append([jnp.concatenate(p, axis=2) for p in zip(*parts)])
    sent_back = []
    for k in range(chunks):
        outs = legendre_stage(
            received[k],
            legendre,
            k,
            mine[k * slots : (k + 1) * slots],
            gather,
            scatter,
            level_cols,
            wave_count,
        )
        if k < chunks - 1:
            outs = [o.reshape(2 * slots, merged * lat_dev) for o in outs]
            sent_back += [swap(o, d, True) for d, o in enumerate(outs)]
    width = merged // last_split
    finals = []
    for q in range(last_split):
        pieces = [
            o[:, :, q * width : (q + 1) * width].reshape(2 * slots, width * lat_dev) for o in outs
        ]
        if q >= 1 and chunks > 1:
            before = finals[q - 2] if q >= 2 else sent_back[-peers:]
            pieces, _ = lax.optimization_barrier((pieces, before[1:]))
        finals.append([swap(o, d, True) for d, o in enumerate(pieces)])
    table = jnp.concatenate(tables, axis=0)
    grid_out = None
    for q in range(last_split):
        grid_out = inverse_fourier(
            sent_back + finals[q], table, merged, lat_dev, last_split, q, grid_out
        )
    return grid_out.reshape(fields, levels, lat_dev, lon_count)


def solution(mesh):
    peers = mesh.shape["wave"]

    def body(*args):
        return per_device(*args, peers=peers)

    in_specs = (
        P("member", "lev", "wave", None),
        P(),
        P(),
        P("wave", None, None, None),
        P(),
        P("member"),
        P("member"),
        P("member"),
    )
    out_specs = P("member", "lev", "wave", None)
    return jax.shard_map(
        body, mesh=mesh, in_specs=in_specs, out_specs=out_specs, check_vma=False
    )
```
